256 devices in a mesh: groups: 2 (over y), expert: 32 (over z, core), dp: 4 (over x).
Axes of the slice: x: 4, y: 2, z: 16, core: 2. Of those that a mesh axis runs over, the one named last changes fastest.
The devices are a block of a 4x16x16 slice.
Arguments:
- tokens: bfloat16 [32768, 2048], P(('groups', 'expert', 'dp')), parts along dimension 0, may hold values from -6 to 6
- expert_ids: int32 [32768, 6], P(('groups', 'expert', 'dp')), parts along dimension 0, may hold values from 0 to 31, all different within a row
- route_weights: float32 [32768, 6], P(('groups', 'expert', 'dp')), parts along dimension 0, may hold values from 0.05 to 0.5
- cotangent: bfloat16 [32768, 2048], P(('groups', 'expert', 'dp')), parts along dimension 0, may hold values from -6 to 6
- in_base: bfloat16 [32, 2, 2048, 704], P('expert'), may hold values from -8 to 8
- in_a: bfloat16 [64, 2, 2048, 16], P(('groups', 'expert')), parts along dimension 0, may hold values from -5 to 5
- in_b: bfloat16 [64, 2, 16, 704], P(('groups', 'expert')), parts along dimension 0, may hold values from -0.75 to 0.75
- in_mag: float32 [64, 2, 704], P(('groups', 'expert')), parts along dimension 0, may hold values from 0.5 to 2
- out_base: bfloat16 [32, 704, 2048], P('expert'), may hold values from -8 to 8
- out_a: bfloat16 [64, 704, 16], P(('groups', 'expert')), parts along dimension 0, may hold values from -5 to 5
- out_b: bfloat16 [64, 16, 2048], P(('groups', 'expert')), parts along dimension 0, may hold values from -0.75 to 0.75
- out_mag: float32 [64, 2048], P(('groups', 'expert')), parts along dimension 0, may hold values from 0.5 to 2
Outputs:
- mixed: bfloat16 [32768, 2048], P(('groups', 'expert', 'dp')), parts along dimension 0
- token_grad: bfloat16 [32768, 2048], P(('groups', 'expert', 'dp')), parts along dimension 0
- route_grad: float32 [32768, 6], P(('groups', 'expert', 'dp')), parts along dimension 0
- in_a_grad: float32 [64, 2, 2048, 16], P(('groups', 'expert')), parts along dimension 0
- in_b_grad: float32 [64, 2, 16, 704], P(('groups', 'expert')), parts along dimension 0
- in_mag_grad: float32 [64, 2, 704], P(('groups', 'expert')), parts along dimension 0
- out_a_grad: float32 [64, 704, 16], P(('groups', 'expert')), parts along dimension 0
- out_b_grad: float32 [64, 16, 2048], P(('groups', 'expert')), parts along dimension 0
- out_mag_grad: float32 [64, 2048], P(('groups', 'expert')), parts along dimension 0
The draws below stay inside these ranges and needn't reach their ends.
There are 2 independent parts, one for each index of `groups`. The reference program is written for one: setup_inputs(seed, part) draws one part's arguments, and reference() takes and returns one part's arrays. A program takes and returns all parts, laid end to end along the dimension named above; an argument that names none is the same for every part. Nothing has to cross between parts.
Inputs may be any that keep to these rules, and one draw needn't show every extreme that they name: `expert_ids`: each row names 6 different experts, and every expert is named by some row.
All inputs are finite; a program needn't handle non-finite values.
Results may differ from the reference program's by a relative error of at most 0.0095.
Values may be sent and summed in bfloat16 or wider, within the bound.
No kernel may reach another device: no remote copies, remote signals or barrier semaphores. Data moves between devices by JAX's collectives and lax.ppermute only.
A program may use at most 128 MiB of HBM per device.

```python
import math
import jax
import jax.numpy as jnp
from jax import lax

D = 2048
FF = 704
RANK = 16
TOK_DEV = 128
EXPERTS = 32
TOP = 6
CAP = 24
TOKENS = 16384


def base_draw(key, leading, fan_in, fan_out):
    key_entry, key_row, key_column = jax.random.split(key, 3)
    layout = leading + (fan_in, fan_out)
    entries = jax.random.normal(key_entry, layout, jnp.float32)
    row_low = 0.3
    row_high = 3.0
    row_scale = jnp.exp(jax.random.uniform(key_row, leading + (fan_in, 1), jnp.float32, math.log(row_low), math.log(row_high)))
    column_scale = jnp.exp(jax.random.uniform(key_column, leading + (1, fan_out), jnp.float32, math.log(0.3), math.log(3.0)))
    return jnp.clip(entries * row_scale * column_scale, -8.0, 8.0).astype(jnp.bfloat16)


def draw_in_base(key, part):
    return base_draw(jax.random.fold_in(key, 11), (EXPERTS, 2), D, FF)


def draw_out_base(key, part):
    return base_draw(jax.random.fold_in(key, 12), (EXPERTS,), FF, D)


def shard_levels(stream_key, shape, cuts, low, high):
    loudness, own = 1.0, jax.random.fold_in(stream_key, 6)
    for position, blocks in cuts:
        steps = jnp.exp(jax.random.uniform(jax.random.fold_in(own, position), (blocks,), jnp.float32, low / len(cuts), high / len(cuts)))
        loudness = loudness * jnp.repeat(steps, shape[position] // blocks).reshape([-1 if axis == position else 1 for axis in range(len(shape))])
    return loudness


def choose_distinct(rng, rows, count, top, lift):
    order = jax.random.permutation(jax.random.fold_in(rng, 1), count)
    boost = order
    for power in range(3):
        boost = boost * boost // count
    boost = boost * lift // count
    lots = jax.random.randint(jax.random.fold_in(rng, 2), (rows, count), 0, 4096) + boost
    holders = jax.random.permutation(jax.random.fold_in(rng, 3), rows)[jnp.arange(count) % rows]
    lots = jnp.where(jnp.arange(rows)[:, None] == holders[None, :], 1 << 14, lots)
    merit = lots * count + jnp.arange(count)
    return lax.top_k(merit.astype(jnp.int32), top)[1].astype(jnp.int32)


def scatter_about(stream_key, extent, width, most, cuts=(), kind=jnp.bfloat16):
    level = shard_levels(stream_key, extent, cuts, -0.22, 0.18) if cuts else 1.0
    drawn = jax.random.normal(stream_key, extent, jnp.float32) * width * level
    return jnp.minimum(jnp.maximum(drawn, -most), most).astype(kind)


def setup_inputs(seed: int = 0, part: int = 0) -> dict:
    splits = jax.random.split(jax.random.key(seed), 13)
    part_splits = jax.random.split(jax.random.fold_in(splits[12], part), 13)
    tokens = scatter_about(part_splits[0], (TOKENS, D), 1.0, 6.0, ((0, 128),))
    expert_ids = choose_distinct(part_splits[1], TOKENS, EXPERTS, TOP, 1536)
    route_weights = jnp.clip(jnp.exp(math.log(0.5) - 2.3025851 * jax.random.uniform(part_splits[2], (TOKENS, TOP), jnp.float32) ** shard_levels(part_splits[2], (TOKENS, TOP), ((0, 128),), -0.2, 0.2)), 0.05, 0.5)
    cotangent = scatter_about(part_splits[3], (TOKENS, D), 1.0, 6.0, ((0, 128),))
    in_base = draw_in_base(jax.random.fold_in(splits[12], 71), part)
    in_a = scatter_about(part_splits[5], (EXPERTS, 2, D, RANK), 1.0, 5.0, ((0, 32),))
    in_b = scatter_about(part_splits[6], (EXPERTS, 2, RANK, FF), (4 * RANK) ** -0.5, 0.75, ((0, 32),))
    in_mag = jnp.clip(jnp.exp(math.log(2.0) - 1.3862944 * jax.random.uniform(part_splits[7], (EXPERTS, 2, FF), jnp.float32) ** shard_levels(part_splits[7], (EXPERTS, 2, FF), ((0, 32),), -0.2, 0.2)), 0.5, 2.0)
    out_base = draw_out_base(jax.random.fold_in(splits[12], 71), part)
    out_a = scatter_about(part_splits[9], (EXPERTS, FF, RANK), 1.0, 5.0, ((0, 32),))
    out_b = scatter_about(part_splits[10], (EXPERTS, RANK, D), (4 * RANK) ** -0.5, 0.75, ((0, 32),))
    out_mag = jnp.clip(jnp.exp(math.log(2.0) - 1.3862944 * jax.random.uniform(part_splits[11], (EXPERTS, D), jnp.float32) ** shard_levels(part_splits[11], (EXPERTS, D), ((0, 32),), -0.2, 0.2)), 0.5, 2.0)
    return dict(tokens=tokens, expert_ids=expert_ids, route_weights=route_weights, cotangent=cotangent, in_base=in_base, in_a=in_a, in_b=in_b, in_mag=in_mag, out_base=out_base, out_a=out_a, out_b=out_b, out_mag=out_mag)


EPS = 1e-06
HIGH = lax.Precision.HIGHEST

def widen(array):
    return array.astype(jnp.float32)

def column_norms(base_weight, low_first, low_second):
    merged = widen(base_weight) + jnp.einsum('...ir,...ro->...io', widen(low_first), widen(low_second), precision=HIGH)
    return jnp.sqrt(lax.optimization_barrier(jnp.sum(merged * merged, axis=-2)) + EPS)

def expert_pass(params, token_rows, cot_rows):
    weights_in, first_in, second_in, mag_in, weights_out, first_out, second_out, mag_out = params
    norm_in = column_norms(weights_in, first_in, second_in)
    scale_in = mag_in / norm_in
    norm_out = column_norms(weights_out, first_out, second_out)
    scale_out = mag_out / norm_out
    low_in = jnp.einsum('nd,pdr->npr', widen(token_rows), widen(first_in), precision=HIGH).astype(jnp.bfloat16)
    raw_in = jnp.einsum('nd,pdf->npf', widen(token_rows), widen(weights_in), precision=HIGH) + jnp.einsum('npr,prf->npf', widen(low_in), widen(second_in), precision=HIGH)
    active = raw_in * scale_in[None]
    gate_act = active[:, 0]
    up_act = active[:, 1]
    sigma = jax.nn.sigmoid(gate_act)
    hidden = (gate_act * sigma * up_act).astype(jnp.bfloat16)
    low_out = jnp.dot(hidden, first_out, preferred_element_type=jnp.float32).astype(jnp.bfloat16)
    raw_out = jnp.dot(hidden, weights_out, preferred_element_type=jnp.float32) + jnp.dot(low_out, second_out, preferred_element_type=jnp.float32)
    result = (raw_out * scale_out).astype(jnp.bfloat16)
    cot_wide = widen(cot_rows)
    grad_out = (cot_wide * scale_out).astype(jnp.bfloat16)
    back_out = jnp.dot(grad_out, second_out.T, preferred_element_type=jnp.float32).astype(jnp.bfloat16)
    hidden_grad = jnp.dot(grad_out, weights_out.T, preferred_element_type=jnp.float32) + jnp.dot(back_out, first_out.T, preferred_element_type=jnp.float32)
    up_grad = hidden_grad * gate_act * sigma
    gate_grad = hidden_grad * up_act * sigma * (1.0 + gate_act * (1.0 - sigma))
    both_grad = jnp.stack([gate_grad, up_grad], axis=1)
    grad_in = (both_grad * scale_in[None]).astype(jnp.bfloat16)
    back_in = jnp.einsum('npf,prf->npr', widen(grad_in), widen(second_in), precision=HIGH).astype(jnp.bfloat16)
    input_grad = (jnp.einsum('npf,pdf->nd', widen(grad_in), widen(weights_in), precision=HIGH) + jnp.einsum('npr,pdr->nd', widen(back_in), widen(first_in), precision=HIGH)).astype(jnp.bfloat16)
    gradients = (jnp.einsum('nd,npr->pdr', widen(token_rows), widen(back_in), precision=HIGH), jnp.einsum('npr,npf->prf', widen(low_in), widen(grad_in), precision=HIGH), lax.optimization_barrier(jnp.sum(both_grad * raw_in, axis=0)) / norm_in, jnp.dot(hidden.T, back_out, preferred_element_type=jnp.float32), jnp.dot(low_out.T, grad_out, preferred_element_type=jnp.float32), lax.optimization_barrier(jnp.sum(cot_wide * raw_out, axis=0)) / norm_out)
    return (result, input_grad, gradients)

def reference(tokens, expert_ids, route_weights, cotangent, in_base, in_a, in_b, in_mag, out_base, out_a, out_b, out_mag):
    blocks = TOKENS // TOK_DEV
    per_block = TOK_DEV * TOP
    flat_ids = expert_ids.reshape(blocks, per_block)
    onehot = (flat_ids[:, :, None] == jnp.arange(EXPERTS, dtype=jnp.int32)[None, None, :]).astype(jnp.int32)
    slots = lax.optimization_barrier(jnp.sum((jnp.cumsum(onehot, axis=1) - onehot) * onehot, axis=-1)).astype(jnp.int32)
    kept = slots < CAP
    block_ids = jnp.arange(blocks, dtype=jnp.int32)[:, None]
    row_pos = (block_ids * CAP + slots).astype(jnp.int32)
    target = jnp.where(kept, flat_ids, EXPERTS).astype(jnp.int32)
    items = jnp.arange(blocks * per_block, dtype=jnp.int32).reshape(blocks, per_block)
    table_width = blocks * CAP
    token_table = jnp.zeros((EXPERTS, table_width), jnp.int32).at[target, row_pos].set(items // TOP, mode='drop')
    item_table = jnp.zeros((EXPERTS, table_width), jnp.int32).at[target, row_pos].set(items, mode='drop')
    weight_table = jnp.zeros((EXPERTS, table_width), jnp.float32).at[target, row_pos].set(route_weights.reshape(blocks, per_block), mode='drop')
    fill_table = jnp.zeros((EXPERTS, table_width), jnp.float32).at[target, row_pos].set(1.0, mode='drop')
    cot_wide = widen(cotangent)

    def per_expert(carry, inputs):
        mixed_sum, grad_sum, route_sum = carry
        token_ids, item_ids, weights_row, fill_row, params = inputs
        token_rows = jnp.where(fill_row[:, None] > 0, tokens[token_ids], jnp.zeros((), tokens.dtype))
        cot_rows = (weights_row[:, None] * cot_wide[token_ids]).astype(jnp.bfloat16)
        result, input_grad, gradients = expert_pass(params, token_rows, cot_rows)
        result_wide = widen(result)
        mixed_sum = mixed_sum.at[token_ids].add(weights_row[:, None] * result_wide)
        grad_sum = grad_sum.at[token_ids].add(fill_row[:, None] * widen(input_grad))
        route_sum = route_sum.at[item_ids].add(fill_row * lax.optimization_barrier(jnp.sum(result_wide * cot_wide[token_ids], axis=-1)))
        return ((mixed_sum, grad_sum, route_sum), gradients)
    start = (jnp.zeros((TOKENS, D), jnp.float32), jnp.zeros((TOKENS, D), jnp.float32), jnp.zeros((TOKENS * TOP,), jnp.float32))
    carried, gradients = lax.scan(per_expert, start, (token_table, item_table, weight_table, fill_table, (in_base, in_a, in_b, in_mag, out_base, out_a, out_b, out_mag)))
    mixed_sum, grad_sum, route_sum = carried
    return (mixed_sum.astype(jnp.bfloat16), grad_sum.astype(jnp.bfloat16), route_sum.reshape(TOKENS, TOP), gradients[0], gradients[1], gradients[2], gradients[3], gradients[4], gradients[5])
```

```python
import jax
import jax.numpy as jnp
from jax import lax
from jax.sharding import PartitionSpec as P

EPS = 1e-06
HIGH = lax.Precision.HIGHEST
CORES = 2
PARTS = 2


def product(pattern, first, second):
    return jnp.einsum(pattern, first, second, preferred_element_type=jnp.float32)


def column_norms(base_weight, low_first, low_second):
    merged = base_weight.astype(jnp.float32) + jnp.einsum(
        "...ir,...ro->...io",
        low_first.astype(jnp.float32),
        low_second.astype(jnp.float32),
        precision=HIGH,
    )
    squares = jnp.sum(merged * merged, axis=-2)
    return jnp.sqrt(squares + EPS)


def forward_rows(token_rows, params):
    weights_in, first_in, second_in, scale_in, weights_out, first_out, second_out, scale_out = (
        params
    )
    low_in = product("nd,pdr->npr", token_rows, first_in).astype(jnp.bfloat16)
    raw_in = product("nd,pdf->npf", token_rows, weights_in) + product(
        "npr,prf->npf", low_in, second_in
    )
    active = raw_in * scale_in[None]
    gate_act = active[:, 0]
    up_act = active[:, 1]
    sigma = jax.nn.sigmoid(gate_act)
    hidden = (gate_act * sigma * up_act).astype(jnp.bfloat16)
    low_out = product("nf,fr->nr", hidden, first_out).astype(jnp.bfloat16)
    raw_out = product("nf,fd->nd", hidden, weights_out) + product("nr,rd->nd", low_out, second_out)
    result = (raw_out * scale_out).astype(jnp.bfloat16)
    return (result, (low_in, raw_in, hidden, low_out, raw_out))


def backward_rows(saved, cot_rows, params):
    weights_in, first_in, second_in, scale_in, weights_out, first_out, second_out, scale_out = (
        params
    )
    low_in, raw_in, hidden, low_out, raw_out = saved
    cot_wide = cot_rows.astype(jnp.float32)
    grad_out = (cot_wide * scale_out).astype(jnp.bfloat16)
    back_out = product("nd,rd->nr", grad_out, second_out).astype(jnp.bfloat16)
    hidden_grad = product("nd,fd->nf", grad_out, weights_out) + product(
        "nr,fr->nf", back_out, first_out
    )
    active = raw_in * scale_in[None]
    gate_act = active[:, 0]
    up_act = active[:, 1]
    sigma = jax.nn.sigmoid(gate_act)
    up_grad = hidden_grad * gate_act * sigma
    gate_grad = hidden_grad * up_act * sigma * (1.0 + gate_act * (1.0 - sigma))
    both_grad = jnp.stack([gate_grad, up_grad], axis=1)
    grad_in = (both_grad * scale_in[None]).astype(jnp.bfloat16)
    back_in = product("npf,prf->npr", grad_in, second_in).astype(jnp.bfloat16)
    input_grad = (
        product("npf,pdf->nd", grad_in, weights_in) + product("npr,pdr->nd", back_in, first_in)
    ).astype(jnp.bfloat16)
    terms = (grad_out, back_out, grad_in, back_in, cot_wide * raw_out, both_grad * raw_in)
    return (input_grad, terms)


class Ring:
    def __init__(self, experts, tok, cap):
        self.size = experts // CORES
        self.half = self.size // 2
        self.tok, self.cap = tok, cap
        short = [h for h in range(2, self.half + 1) if self.rows(h) < tok]
        self.packed = min(short) if short else self.half + 1

    def rows(self, h):
        return min(self.tok, self.cap * (1 + CORES * (self.half - h)))

    def shift(self, array, step):
        pairs = [
            (CORES * z + c, CORES * ((z + step) % self.size) + c)
            for z in range(self.size)
            for c in range(CORES)
        ]
        return lax.ppermute(array, "expert", pairs)

    def swap(self, array):
        pairs = [
            (CORES * z + c, CORES * z + CORES - 1 - c)
            for z in range(self.size)
            for c in range(CORES)
        ]
        return lax.ppermute(array, "expert", pairs)

    def source(self, step, h):
        return (step * h) % self.size


def route_tables(ring, expert_ids, route_weights, me):
    tok, top = expert_ids.shape
    experts = ring.size * CORES
    every = jnp.arange(experts, dtype=jnp.int32)
    named = expert_ids.T[None, :, :] == every[:, None, None]
    hit = jnp.any(named, axis=1)
    weight = jnp.sum(jnp.where(named, route_weights.T[None], 0.0), axis=1)
    row = jnp.arange(tok, dtype=jnp.int32)
    earlier = (row[:, None] < row[None, :]).astype(jnp.bfloat16)
    slot = product("et,ts->es", hit.astype(jnp.bfloat16), earlier).astype(jnp.int32)
    kept = hit & (slot < ring.cap)
    ahead = (every // CORES - me // CORES) % ring.size
    first_core = every % CORES == 0
    forward = (ahead < ring.half) | ((ahead == ring.half) & first_core)
    far = jnp.where(forward, ahead, ring.size - ahead)

    def ranks(mine):
        key = jnp.max(jnp.where(kept & mine[:, None], far[:, None], 0), axis=0)
        before = (key[:, None] > key[None, :]) | (
            (key[:, None] == key[None, :]) & (row[:, None] < row[None, :])
        )
        return jnp.sum(before.astype(jnp.int32), axis=0)

    rank_forward = ranks(forward)
    rank_backward = ranks(~forward)
    rank = jnp.where(forward[:, None], rank_forward[None], rank_backward[None])
    place = jnp.where((far >= ring.packed)[:, None], rank, row[None])
    place = place + jnp.where((far == ring.half) & ~forward, ring.cap, 0)[:, None]
    slots = jnp.arange(ring.cap, dtype=jnp.int32)
    held = kept[:, None, :] & (slot[:, None, :] == slots[None, :, None])
    where = jnp.sum(jnp.where(held, place[:, None, :] + 1, 0), axis=2) - 1
    weights = jnp.sum(jnp.where(held, weight[:, None, :], 0.0), axis=2)
    pairs = jnp.repeat(where.reshape(ring.size, CORES * ring.cap), CORES, axis=0)
    table = jnp.concatenate(
        [pairs.astype(jnp.float32), weights, rank.astype(jnp.float32)], axis=1
    )
    return table, slot, kept


def spread(ring, part, orders):
    came = {}
    for step in (1, -1):
        cur = part
        for h in range(1, ring.half + 1):
            if h == ring.packed:
                cur = product("pt,td->pd", orders[step], cur).astype(jnp.bfloat16)
            elif ring.rows(h) < cur.shape[0]:
                cur = cur[: ring.rows(h)]
            cur = ring.shift(cur, step)
            came[step, h] = cur
    return came


def pick(ring, part, came, choose):
    picked = []
    for back in range(ring.size):
        if back == 0:
            block = part
        elif back == ring.half:
            block = jnp.concatenate([came[1, ring.half], came[-1, ring.half]], axis=0)
        elif back < ring.half:
            block = came[1, back]
        else:
            block = came[-1, ring.size - back]
        chosen = choose[back][:, : block.shape[0]]
        picked.append(product("st,td->sd", chosen, block).astype(jnp.bfloat16))
    return jnp.stack(picked)


def gather_sums(ring, part, choose, orders):
    both = []
    for step in (1, -1):
        came = None
        for h in range(ring.half, 0, -1):
            back = (step * h) % ring.size
            count = ring.rows(h)
            chosen = choose[back]
            if h == ring.half:
                first = 0 if step == 1 else count
                chosen = chosen[:, first : first + count]
            else:
                chosen = chosen[:, :count]
            total = product("st,sd->td", chosen, part[back])
            if came is not None:
                if h == ring.packed - 1:
                    total = total + product("pt,pd->td", orders[step], came)
                else:
                    wide = came.astype(jnp.float32)
                    total = total + jnp.pad(wide, ((0, count - wide.shape[0]), (0, 0)))
            came = ring.shift(total.astype(jnp.bfloat16), -step)
        both.append(came.astype(jnp.float32))
    local = product("st,sd->td", choose[0], part[0])
    return (local + both[0] + both[1]).astype(jnp.bfloat16)


def columns(array):
    return jnp.split(array, PARTS, axis=-1)


def per_device(
    tokens,
    expert_ids,
    route_weights,
    cotangent,
    in_base,
    in_a,
    in_b,
    in_mag,
    out_base,
    out_a,
    out_b,
    out_mag,
):
    experts = lax.axis_size("expert")
    tok, top = expert_ids.shape
    width = tokens.shape[1]
    cap = tok * top // experts
    ring = Ring(experts, tok, cap)
    size = ring.size
    me = lax.axis_index("expert")
    z, core = me // CORES, me % CORES

    table, slot, kept = route_tables(ring, expert_ids, route_weights, me)
    got = lax.all_to_all(
        table[:, None, :], "expert", split_axis=0, concat_axis=0, tiled=True
    )[:, 0]
    back = (z - jnp.arange(size, dtype=jnp.int32)) % size
    mine = got[back * CORES + core]
    other = got[back * CORES + 1 - core]
    places = mine[:, : CORES * cap].astype(jnp.int32)
    low, high = places[:, :cap], places[:, cap:]
    places = jnp.concatenate(
        [jnp.where(core == 0, low, high), jnp.where(core == 0, high, low)], axis=1
    )
    spots = jnp.arange(tok, dtype=jnp.int32)
    choose = (places[:, :, None] == spots[None, None, :]).astype(jnp.bfloat16)
    row_weights = jnp.concatenate(
        [
            mine[:, CORES * cap : (CORES + 1) * cap].reshape(-1),
            other[:, CORES * cap : (CORES + 1) * cap].reshape(-1),
        ]
    )
    ranks = mine[:, (CORES + 1) * cap :].astype(jnp.int32)
    orders = {}
    if ring.packed <= ring.half:
        span = jnp.arange(ring.rows(ring.packed), dtype=jnp.int32)
        for step in (1, -1):
            rank = ranks[(step * (ring.packed - 1)) % size]
            orders[step] = (rank[None, :] == span[:, None]).astype(jnp.bfloat16)

    token_parts = columns(tokens)
    token_came = [spread(ring, part, orders) for part in token_parts]
    gate = min(max(1, ring.packed - 1), ring.half)
    cot_parts = [
        lax.optimization_barrier((part, came[1, gate], came[-1, gate]))[0]
        for part, came in zip(columns(cotangent), token_came)
    ]
    cot_came = [spread(ring, part, orders) for part in cot_parts]

    def arrive(parts, came):
        rows = jnp.concatenate(
            [pick(ring, part, c, choose) for part, c in zip(parts, came)], axis=-1
        )
        own = rows[:, :cap].reshape(size * cap, width)
        sent = ring.swap(rows[:, cap:].reshape(size * cap, width))
        return jnp.concatenate([own, sent], axis=0)

    def leave(rows):
        own = rows[: size * cap].reshape(size, cap, width)
        swapped = ring.swap(rows[size * cap :]).reshape(size, cap, width)
        both = jnp.concatenate([own, swapped], axis=1)
        return jnp.concatenate(
            [gather_sums(ring, part, choose, orders) for part in columns(both)], axis=-1
        )

    norm_in = column_norms(in_base[0], in_a[0], in_b[0])
    norm_out = column_norms(out_base[0], out_a[0], out_b[0])
    params = (
        in_base[0],
        in_a[0],
        in_b[0],
        in_mag[0] / norm_in,
        out_base[0],
        out_a[0],
        out_b[0],
        out_mag[0] / norm_out,
    )

    token_rows = arrive(token_parts, token_came)
    result, saved = forward_rows(token_rows, params)
    mixed = leave((row_weights[:, None] * result.astype(jnp.float32)).astype(jnp.bfloat16))

    raw_cot = arrive(cot_parts, cot_came).astype(jnp.float32)
    cot_rows = (row_weights[:, None] * raw_cot).astype(jnp.bfloat16)
    input_grad, terms = backward_rows(saved, cot_rows, params)
    token_grad = leave(input_grad)

    row_grad = jnp.sum(result.astype(jnp.float32) * raw_cot, axis=-1).reshape(CORES, size, cap)
    ahead = (z - jnp.arange(size, dtype=jnp.int32)) % size
    by_core = jnp.stack(
        [
            jnp.where(core == 0, row_grad[0], row_grad[1]),
            jnp.where(core == 0, row_grad[1], row_grad[0]),
        ],
        axis=1,
    )[ahead].reshape(experts, 1, cap)
    returned = lax.all_to_all(by_core, "expert", split_axis=0, concat_axis=0, tiled=True)[:, 0]
    slots = jnp.arange(cap, dtype=jnp.int32)
    held = kept[:, :, None] & (slot[:, :, None] == slots[None, None, :])
    per_pair = jnp.sum(jnp.where(held, returned[:, None, :], 0.0), axis=2)
    every = jnp.arange(experts, dtype=jnp.int32)
    named = expert_ids[:, :, None] == every[None, None, :]
    route_grad = jnp.sum(jnp.where(named, per_pair.T[:, None, :], 0.0), axis=2)

    low_in, raw_in, hidden, low_out, raw_out = saved
    grad_out, back_out, grad_in, back_in, out_mag_rows, in_mag_rows = terms
    in_a_grad = product("nd,npr->pdr", token_rows, back_in)
    in_b_grad = product("npr,npf->prf", low_in, grad_in)
    in_mag_grad = jnp.sum(in_mag_rows, axis=0) / norm_in
    out_a_grad = product("nf,nr->fr", hidden, back_out)
    out_b_grad = product("nr,nd->rd", low_out, grad_out)
    out_mag_grad = jnp.sum(out_mag_rows, axis=0) / norm_out
    grads = (in_a_grad, in_b_grad, in_mag_grad, out_a_grad, out_b_grad, out_mag_grad)
    summed = [lax.psum(g.astype(jnp.bfloat16), "dp").astype(jnp.float32)[None] for g in grads]
    return (mixed, token_grad, route_grad, *summed)


def solution(mesh):
    in_specs = (
        P(("groups", "expert", "dp"), None),
        P(("groups", "expert", "dp"), None),
        P(("groups", "expert", "dp"), None),
        P(("groups", "expert", "dp"), None),
        P("expert", None, None, None),
        P(("groups", "expert"), None, None, None),
        P(("groups", "expert"), None, None, None),
        P(("groups", "expert"), None, None),
        P("expert", None, None),
        P(("groups", "expert"), None, None),
        P(("groups", "expert"), None, None),
        P(("groups", "expert"), None),
    )
    out_specs = (
        P(("groups", "expert", "dp"), None),
        P(("groups", "expert", "dp"), None),
        P(("groups", "expert", "dp"), None),
        P(("groups", "expert"), None, None, None),
        P(("groups", "expert"), None, None, None),
        P(("groups", "expert"), None, None),
        P(("groups", "expert"), None, None),
        P(("groups", "expert"), None, None),
        P(("groups", "expert"), None),
    )
    return jax.shard_map(
        per_device, mesh=mesh, in_specs=in_specs, out_specs=out_specs, check_vma=False
    )
```

```python
import jax
import jax.numpy as jnp
from jax import lax
from jax.sharding import PartitionSpec as P

EPS = 1e-06
HIGH = lax.Precision.HIGHEST
CORES = 2
PARTS = 2


def product(pattern, first, second):
    return jnp.einsum(pattern, first, second, preferred_element_type=jnp.float32)


def column_norms(base_weight, low_first, low_second):
    merged = base_weight.astype(jnp.float32) + jnp.einsum(
        "...ir,...ro->...io",
        low_first.astype(jnp.float32),
        low_second.astype(jnp.float32),
        precision=HIGH,
    )
    squares = jnp.sum(merged * merged, axis=-2)
    return jnp.sqrt(squares + EPS)


def forward_rows(token_rows, params):
    weights_in, first_in, second_in, scale_in, weights_out, first_out, second_out, scale_out = (
        params
    )
    low_in = product("nd,pdr->npr", token_rows, first_in).astype(jnp.bfloat16)
    raw_in = product("nd,pdf->npf", token_rows, weights_in) + product(
        "npr,prf->npf", low_in, second_in
    )
    active = raw_in * scale_in[None]
    gate_act = active[:, 0]
    up_act = active[:, 1]
    sigma = jax.nn.sigmoid(gate_act)
    hidden = (gate_act * sigma * up_act).astype(jnp.bfloat16)
    low_out = product("nf,fr->nr", hidden, first_out).astype(jnp.bfloat16)
    raw_out = product("nf,fd->nd", hidden, weights_out) + product("nr,rd->nd", low_out, second_out)
    result = (raw_out * scale_out).astype(jnp.bfloat16)
    return (result, (low_in, raw_in, hidden, low_out, raw_out))


def backward_rows(saved, cot_rows, params):
    weights_in, first_in, second_in, scale_in, weights_out, first_out, second_out, scale_out = (
        params
    )
    low_in, raw_in, hidden, low_out, raw_out = saved
    cot_wide = cot_rows.astype(jnp.float32)
    grad_out = (cot_wide * scale_out).astype(jnp.bfloat16)
    back_out = product("nd,rd->nr", grad_out, second_out).astype(jnp.bfloat16)
    hidden_grad = product("nd,fd->nf", grad_out, weights_out) + product(
        "nr,fr->nf", back_out, first_out
    )
    active = raw_in * scale_in[None]
    gate_act = active[:, 0]
    up_act = active[:, 1]
    sigma = jax.nn.sigmoid(gate_act)
    up_grad = hidden_grad * gate_act * sigma
    gate_grad = hidden_grad * up_act * sigma * (1.0 + gate_act * (1.0 - sigma))
    both_grad = jnp.stack([gate_grad, up_grad], axis=1)
    grad_in = (both_grad * scale_in[None]).astype(jnp.bfloat16)
    back_in = product("npf,prf->npr", grad_in, second_in).astype(jnp.bfloat16)
    input_grad = (
        product("npf,pdf->nd", grad_in, weights_in) + product("npr,pdr->nd", back_in, first_in)
    ).astype(jnp.bfloat16)
    terms = (grad_out, back_out, grad_in, back_in, cot_wide * raw_out, both_grad * raw_in)
    return (input_grad, terms)


class Ring:
    def __init__(self, experts, tok, cap):
        self.size = experts // CORES
        self.half = self.size // 2
        self.tok, self.cap = tok, cap
        short = [h for h in range(2, self.half + 1) if self.rows(h) < tok]
        self.packed = min(short) if short else self.half + 1

    def rows(self, h):
        return min(self.tok, self.cap * (1 + CORES * (self.half - h)))

    def shift(self, array, step):
        pairs = [
            (CORES * z + c, CORES * ((z + step) % self.size) + c)
            for z in range(self.size)
            for c in range(CORES)
        ]
        return lax.ppermute(array, "expert", pairs)

    def swap(self, array):
        pairs = [
            (CORES * z + c, CORES * z + CORES - 1 - c)
            for z in range(self.size)
            for c in range(CORES)
        ]
        return lax.ppermute(array, "expert", pairs)

    def source(self, step, h):
        return (step * h) % self.size


def route_tables(ring, expert_ids, route_weights, me):
    tok, top = expert_ids.shape
    experts = ring.size * CORES
    every = jnp.arange(experts, dtype=jnp.int32)
    named = expert_ids.T[None, :, :] == every[:, None, None]
    hit = jnp.any(named, axis=1)
    weight = jnp.sum(jnp.where(named, route_weights.T[None], 0.0), axis=1)
    row = jnp.arange(tok, dtype=jnp.int32)
    earlier = (row[:, None] < row[None, :]).astype(jnp.bfloat16)
    slot = product("et,ts->es", hit.astype(jnp.bfloat16), earlier).astype(jnp.int32)
    kept = hit & (slot < ring.cap)
    ahead = (every // CORES - me // CORES) % ring.size
    first_core = every % CORES == 0
    forward = (ahead < ring.half) | ((ahead == ring.half) & first_core)
    far = jnp.where(forward, ahead, ring.size - ahead)

    def ranks(mine):
        key = jnp.max(jnp.where(kept & mine[:, None], far[:, None], 0), axis=0)
        before = (key[:, None] > key[None, :]) | (
            (key[:, None] == key[None, :]) & (row[:, None] < row[None, :])
        )
        return jnp.sum(before.astype(jnp.int32), axis=0)

    rank_forward = ranks(forward)
    rank_backward = ranks(~forward)
    rank = jnp.where(forward[:, None], rank_forward[None], rank_backward[None])
    place = jnp.where((far >= ring.packed)[:, None], rank, row[None])
    place = place + jnp.where((far == ring.half) & ~forward, ring.cap, 0)[:, None]
    slots = jnp.arange(ring.cap, dtype=jnp.int32)
    held = kept[:, None, :] & (slot[:, None, :] == slots[None, :, None])
    where = jnp.sum(jnp.where(held, place[:, None, :] + 1, 0), axis=2) - 1
    weights = jnp.sum(jnp.where(held, weight[:, None, :], 0.0), axis=2)
    pairs = jnp.repeat(where.reshape(ring.size, CORES * ring.cap), CORES, axis=0)
    table = jnp.concatenate(
        [pairs.astype(jnp.float32), weights, rank.astype(jnp.float32)], axis=1
    )
    return table, slot, kept


def after(array, *others):
    return lax.optimization_barrier((array, *others))[0]


class Spread:
    def __init__(self, ring, parts):
        self.ring, self.parts = ring, parts
        self.now = {(i, step): part for i, part in enumerate(parts) for step in (1, -1)}
        self.came = {}

    def hop(self, h, orders=None, wait=()):
        ring = self.ring
        for (i, step), cur in self.now.items():
            if h == ring.packed:
                cur = product("pt,td->pd", orders[step], cur).astype(jnp.bfloat16)
            elif ring.rows(h) < cur.shape[0]:
                cur = cur[: ring.rows(h)]
            if wait:
                cur = after(cur, *wait)
            cur = ring.shift(cur, step)
            self.now[i, step] = cur
            self.came[i, step, h] = cur

    def at(self, h):
        return tuple(self.came[i, step, h] for (i, step) in self.now)

    def pick(self, choose):
        ring = self.ring
        halves = []
        for i, part in enumerate(self.parts):
            picked = []
            for back in range(ring.size):
                if back == 0:
                    block = part
                elif back == ring.half:
                    block = jnp.concatenate(
                        [self.came[i, 1, ring.half], self.came[i, -1, ring.half]], axis=0
                    )
                elif back < ring.half:
                    block = self.came[i, 1, back]
                else:
                    block = self.came[i, -1, ring.size - back]
                chosen = choose[back][:, : block.shape[0]]
                picked.append(product("st,td->sd", chosen, block).astype(jnp.bfloat16))
            halves.append(jnp.stack(picked))
        return jnp.concatenate(halves, axis=-1)


class Collect:
    def __init__(self, ring, rows, choose, orders, batch):
        self.ring, self.choose, self.orders = ring, choose, orders
        self.parts = columns(rows)
        self.now = {(i, step): None for i in range(len(self.parts)) for step in (1, -1)}
        self.came = {}
        self.ready = None
        if batch:
            terms = product("bst,bsd->btd", choose, rows).astype(jnp.bfloat16)
            self.ready = [columns(terms[back]) for back in range(ring.size)]

    def term(self, i, back, first, count):
        if self.ready is not None:
            return self.ready[back][i][first : first + count].astype(jnp.float32)
        chosen = self.choose[back][:, first : first + count]
        return product("st,sd->td", chosen, self.parts[i][back])

    def hop(self, h, wait=()):
        ring = self.ring
        for (i, step), came in self.now.items():
            count = ring.rows(h)
            first = count if h == ring.half and step == -1 else 0
            total = self.term(i, (step * h) % ring.size, first, count)
            if came is not None:
                if h == ring.packed - 1:
                    total = total + product("pt,pd->td", self.orders[step], came)
                else:
                    wide = came.astype(jnp.float32)
                    total = total + jnp.pad(wide, ((0, count - wide.shape[0]), (0, 0)))
            total = total.astype(jnp.bfloat16)
            if wait:
                total = after(total, *wait)
            came = ring.shift(total, -step)
            self.now[i, step] = came
            self.came[i, step, h] = came

    def at(self, h):
        return tuple(self.came[i, step, h] for (i, step) in self.now)

    def result(self):
        done = []
        for i in range(len(self.parts)):
            local = self.term(i, 0, 0, self.ring.tok)
            both = self.now[i, 1].astype(jnp.float32) + self.now[i, -1].astype(jnp.float32)
            done.append((local + both).astype(jnp.bfloat16))
        return jnp.concatenate(done, axis=-1)


def exchange(array, mask):
    count = lax.axis_size("dp")
    return lax.ppermute(array, "dp", [(x, x ^ mask) for x in range(count)])


def columns(array):
    return jnp.split(array, PARTS, axis=-1)


def per_device(
    tokens,
    expert_ids,
    route_weights,
    cotangent,
    in_base,
    in_a,
    in_b,
    in_mag,
    out_base,
    out_a,
    out_b,
    out_mag,
):
    experts = lax.axis_size("expert")
    tok, top = expert_ids.shape
    width = tokens.shape[1]
    cap = tok * top // experts
    ring = Ring(experts, tok, cap)
    size = ring.size
    me = lax.axis_index("expert")
    z, core = me // CORES, me % CORES

    tok_ring = Spread(ring, columns(tokens))
    tok_ring.hop(1)
    table, slot, kept = route_tables(ring, expert_ids, route_weights, me)
    got = lax.all_to_all(
        table[:, None, :], "expert", split_axis=0, concat_axis=0, tiled=True
    )[:, 0]
    tok_ring.hop(2)
    got = after(got, *tok_ring.at(2))
    back = (z - jnp.arange(size, dtype=jnp.int32)) % size
    mine = got[back * CORES + core]
    other = got[back * CORES + 1 - core]
    places = mine[:, : CORES * cap].astype(jnp.int32)
    low, high = places[:, :cap], places[:, cap:]
    places = jnp.concatenate(
        [jnp.where(core == 0, low, high), jnp.where(core == 0, high, low)], axis=1
    )
    spots = jnp.arange(tok, dtype=jnp.int32)
    choose = (places[:, :, None] == spots[None, None, :]).astype(jnp.bfloat16)
    row_weights = jnp.concatenate(
        [
            mine[:, CORES * cap : (CORES + 1) * cap].reshape(-1),
            other[:, CORES * cap : (CORES + 1) * cap].reshape(-1),
        ]
    )
    ranks = mine[:, (CORES + 1) * cap :].astype(jnp.int32)
    span = jnp.arange(ring.rows(ring.packed), dtype=jnp.int32)
    orders = {
        step: (ranks[(step * (ring.packed - 1)) % size][None, :] == span[:, None]).astype(
            jnp.bfloat16
        )
        for step in (1, -1)
    }

    def swapped_in(picked):
        own = picked[:, :cap].reshape(size * cap, width)
        sent = ring.swap(picked[:, cap:].reshape(size * cap, width))
        return jnp.concatenate([own, sent], axis=0)

    def swapped_out(rows):
        own = rows[: size * cap].reshape(size, cap, width)
        swapped = ring.swap(rows[size * cap :]).reshape(size, cap, width)
        return jnp.concatenate([own, swapped], axis=1)

    tok_ring.hop(3)
    weights_in = after(in_base[0], *tok_ring.at(3))
    weights_out = after(out_base[0], *tok_ring.at(3))
    norm_in = column_norms(weights_in, in_a[0], in_b[0])
    norm_out = column_norms(weights_out, out_a[0], out_b[0])
    params = (
        weights_in,
        in_a[0],
        in_b[0],
        in_mag[0] / norm_in,
        weights_out,
        out_a[0],
        out_b[0],
        out_mag[0] / norm_out,
    )
    for h in range(4, ring.packed + 1):
        tok_ring.hop(h, orders)
    cot_ring = Spread(ring, columns(after(cotangent, *tok_ring.at(ring.packed))))
    ahead = 0
    for h in range(ring.packed + 1, ring.half + 1):
        tok_ring.hop(h)
        ahead += 1
        cot_ring.hop(ahead)

    token_rows = swapped_in(tok_ring.pick(choose))
    result, saved = forward_rows(token_rows, params)
    hidden = saved[2]
    weighted = (row_weights[:, None] * result.astype(jnp.float32)).astype(jnp.bfloat16)
    mix_ring = Collect(ring, swapped_out(weighted), choose, orders, True)
    cot_ring.hop(3)
    cot_ring.hop(4, wait=(hidden,))
    cot_ring.hop(5, wait=(mix_ring.ready[size // 2][0],))
    cot_ring.hop(6, orders)
    mix_ring.hop(8)
    cot_ring.hop(7, wait=mix_ring.at(8))
    mix_ring.hop(7)
    cot_ring.hop(8, wait=mix_ring.at(7))
    mix_ring.hop(6)
    mix_ring.hop(5)
    mix_ring.hop(4)

    raw_cot = swapped_in(cot_ring.pick(choose)).astype(jnp.float32)
    cot_rows = (row_weights[:, None] * raw_cot).astype(jnp.bfloat16)
    input_grad, terms = backward_rows(saved, cot_rows, params)
    mix_ring.hop(3, wait=(terms[2],))
    grad_rows = swapped_out(input_grad)
    mix_ring.hop(2, wait=(grad_rows,))
    grad_ring = Collect(ring, grad_rows, choose, orders, False)
    grad_ring.hop(8)
    mix_ring.hop(1, wait=grad_ring.at(8))

    row_grad = jnp.sum(result.astype(jnp.float32) * raw_cot, axis=-1).reshape(CORES, size, cap)
    by_core = jnp.stack(
        [
            jnp.where(core == 0, row_grad[0], row_grad[1]),
            jnp.where(core == 0, row_grad[1], row_grad[0]),
        ],
        axis=1,
    )[back].reshape(experts, 1, cap)
    returned = lax.all_to_all(by_core, "expert", split_axis=0, concat_axis=0, tiled=True)[:, 0]
    slots = jnp.arange(cap, dtype=jnp.int32)
    held = kept[:, :, None] & (slot[:, :, None] == slots[None, None, :])
    per_pair = jnp.sum(jnp.where(held, returned[:, None, :], 0.0), axis=2)
    every = jnp.arange(experts, dtype=jnp.int32)
    named = expert_ids[:, :, None] == every[None, None, :]
    route_grad = jnp.sum(jnp.where(named, per_pair.T[:, None, :], 0.0), axis=2)

    for h in (7, 6, 5):
        grad_ring.hop(h)
    low_in, raw_in, hidden, low_out, raw_out = saved
    grad_out, back_out, grad_in, back_in, out_mag_rows, in_mag_rows = terms
    rank, inner = in_b.shape[2], in_b.shape[3]
    wide = jnp.concatenate(
        [
            product("nd,npr->prd", token_rows, back_in).reshape(-1, width),
            product("nr,nd->rd", low_out, grad_out),
            (jnp.sum(out_mag_rows, axis=0) / norm_out)[None],
        ],
        axis=0,
    ).astype(jnp.bfloat16)
    slim = jnp.concatenate(
        [
            product("npr,npf->prf", low_in, grad_in).reshape(-1, inner),
            product("nf,nr->rf", hidden, back_out),
            jnp.sum(in_mag_rows, axis=0) / norm_in,
        ],
        axis=0,
    ).astype(jnp.bfloat16)
    grad_ring.hop(4, wait=(wide, slim))
    order = [4, 3, 2, 1]
    mask = 1
    while mask < lax.axis_size("dp"):
        add_wide, add_slim = exchange(wide, mask), exchange(slim, mask)
        wide = wide.astype(jnp.float32) + add_wide.astype(jnp.float32)
        slim = slim.astype(jnp.float32) + add_slim.astype(jnp.float32)
        mask = 2 * mask + 1
        if mask < lax.axis_size("dp"):
            wide, slim = wide.astype(jnp.bfloat16), slim.astype(jnp.bfloat16)
            grad_ring.hop(3, wait=(add_wide, add_slim))
    grad_ring.hop(2)
    grad_ring.hop(1, wait=(add_wide, add_slim))
    pairs = CORES * rank
    summed = (
        wide[:pairs].reshape(2, rank, width).transpose(0, 2, 1),
        slim[:pairs].reshape(2, rank, inner),
        slim[-2:],
        slim[pairs : pairs + rank].T,
        wide[pairs : pairs + rank],
        wide[-1],
    )
    return (
        mix_ring.result(),
        grad_ring.result(),
        route_grad,
        *(array[None] for array in summed),
    )


def solution(mesh):
    in_specs = (
        P(("groups", "expert", "dp"), None),
        P(("groups", "expert", "dp"), None),
        P(("groups", "expert", "dp"), None),
        P(("groups", "expert", "dp"), None),
        P("expert", None, None, None),
        P(("groups", "expert"), None, None, None),
        P(("groups", "expert"), None, None, None),
        P(("groups", "expert"), None, None),
        P("expert", None, None),
        P(("groups", "expert"), None, None),
        P(("groups", "expert"), None, None),
        P(("groups", "expert"), None),
    )
    out_specs = (
        P(("groups", "expert", "dp"), None),
        P(("groups", "expert", "dp"), None),
        P(("groups", "expert", "dp"), None),
        P(("groups", "expert"), None, None, None),
        P(("groups", "expert"), None, None, None),
        P(("groups", "expert"), None, None),
        P(("groups", "expert"), None, None),
        P(("groups", "expert"), None, None),
        P(("groups", "expert"), None),
    )
    return jax.shard_map(
        per_device, mesh=mesh, in_specs=in_specs, out_specs=out_specs, check_vma=False
    )
```

```python
import jax
import jax.numpy as jnp
from jax import lax
from jax.sharding import PartitionSpec as P

EPS = 1e-06
HIGH = lax.Precision.HIGHEST
CORES = 2
PARTS = 2


def product(pattern, first, second):
    return jnp.einsum(pattern, first, second, preferred_element_type=jnp.float32)


def column_norms(base_weight, low_first, low_second):
    merged = base_weight.astype(jnp.float32) + jnp.einsum(
        "...ir,...ro->...io",
        low_first.astype(jnp.float32),
        low_second.astype(jnp.float32),
        precision=HIGH,
    )
    squares = jnp.sum(merged * merged, axis=-2)
    return jnp.sqrt(squares + EPS)


def forward_rows(token_rows, params):
    weights_in, first_in, second_in, scale_in, weights_out, first_out, second_out, scale_out = (
        params
    )
    low_in = product("nd,pdr->npr", token_rows, first_in).astype(jnp.bfloat16)
    raw_in = product("nd,pdf->npf", token_rows, weights_in) + product(
        "npr,prf->npf", low_in, second_in
    )
    active = raw_in * scale_in[None]
    gate_act = active[:, 0]
    up_act = active[:, 1]
    sigma = jax.nn.sigmoid(gate_act)
    hidden = (gate_act * sigma * up_act).astype(jnp.bfloat16)
    low_out = product("nf,fr->nr", hidden, first_out).astype(jnp.bfloat16)
    raw_out = product("nf,fd->nd", hidden, weights_out) + product("nr,rd->nd", low_out, second_out)
    result = (raw_out * scale_out).astype(jnp.bfloat16)
    return (result, (low_in, raw_in, hidden, low_out, raw_out))


def backward_rows(saved, cot_rows, params, mix_ring):
    weights_in, first_in, second_in, scale_in, weights_out, first_out, second_out, scale_out = (
        params
    )
    low_in, raw_in, hidden, low_out, raw_out = saved
    cot_wide = cot_rows.astype(jnp.float32)
    grad_out = (cot_wide * scale_out).astype(jnp.bfloat16)
    back_out = product("nd,rd->nr", grad_out, second_out).astype(jnp.bfloat16)
    hidden_grad = product("nd,fd->nf", grad_out, weights_out) + product(
        "nr,fr->nf", back_out, first_out
    )
    mix_ring.hop(5, wait=(hidden_grad,))
    active = raw_in * scale_in[None]
    gate_act = active[:, 0]
    up_act = active[:, 1]
    sigma = jax.nn.sigmoid(gate_act)
    up_grad = hidden_grad * gate_act * sigma
    gate_grad = hidden_grad * up_act * sigma * (1.0 + gate_act * (1.0 - sigma))
    both_grad = jnp.stack([gate_grad, up_grad], axis=1)
    grad_in = (both_grad * scale_in[None]).astype(jnp.bfloat16)
    back_in = product("npf,prf->npr", grad_in, second_in).astype(jnp.bfloat16)
    mix_ring.hop(4, wait=(grad_in,))
    input_grad = (
        product("npf,pdf->nd", grad_in, weights_in) + product("npr,pdr->nd", back_in, first_in)
    ).astype(jnp.bfloat16)
    terms = (grad_out, back_out, grad_in, back_in, cot_wide * raw_out, both_grad * raw_in)
    return (input_grad, terms)


class Ring:
    def __init__(self, experts, tok, cap):
        self.size = experts // CORES
        self.half = self.size // 2
        self.tok, self.cap = tok, cap
        short = [h for h in range(2, self.half + 1) if self.rows(h) < tok]
        self.packed = min(short) if short else self.half + 1

    def rows(self, h):
        return min(self.tok, self.cap * (1 + CORES * (self.half - h)))

    def shift(self, array, step):
        pairs = [
            (CORES * z + c, CORES * ((z + step) % self.size) + c)
            for z in range(self.size)
            for c in range(CORES)
        ]
        return lax.ppermute(array, "expert", pairs)

    def swap(self, array):
        pairs = [
            (CORES * z + c, CORES * z + CORES - 1 - c)
            for z in range(self.size)
            for c in range(CORES)
        ]
        return lax.ppermute(array, "expert", pairs)

    def source(self, step, h):
        return (step * h) % self.size


def route_tables(ring, expert_ids, route_weights, me):
    tok, top = expert_ids.shape
    experts = ring.size * CORES
    every = jnp.arange(experts, dtype=jnp.int32)
    named = expert_ids.T[None, :, :] == every[:, None, None]
    hit = jnp.any(named, axis=1)
    weight = jnp.sum(jnp.where(named, route_weights.T[None], 0.0), axis=1)
    row = jnp.arange(tok, dtype=jnp.int32)
    earlier = (row[:, None] < row[None, :]).astype(jnp.bfloat16)
    slot = product("et,ts->es", hit.astype(jnp.bfloat16), earlier).astype(jnp.int32)
    kept = hit & (slot < ring.cap)
    ahead = (every // CORES - me // CORES) % ring.size
    first_core = every % CORES == 0
    forward = (ahead < ring.half) | ((ahead == ring.half) & first_core)
    far = jnp.where(forward, ahead, ring.size - ahead)

    def ranks(mine):
        key = jnp.max(jnp.where(kept & mine[:, None], far[:, None], 0), axis=0)
        before = (key[:, None] > key[None, :]) | (
            (key[:, None] == key[None, :]) & (row[:, None] < row[None, :])
        )
        return jnp.sum(before.astype(jnp.int32), axis=0)

    rank_forward = ranks(forward)
    rank_backward = ranks(~forward)
    rank = jnp.where(forward[:, None], rank_forward[None], rank_backward[None])
    place = jnp.where((far >= ring.packed)[:, None], rank, row[None])
    place = place + jnp.where((far == ring.half) & ~forward, ring.cap, 0)[:, None]
    slots = jnp.arange(ring.cap, dtype=jnp.int32)
    held = kept[:, None, :] & (slot[:, None, :] == slots[None, :, None])
    where = jnp.sum(jnp.where(held, place[:, None, :] + 1, 0), axis=2) - 1
    weights = jnp.sum(jnp.where(held, weight[:, None, :], 0.0), axis=2)
    pairs = jnp.repeat(where.reshape(ring.size, CORES * ring.cap), CORES, axis=0)
    table = jnp.concatenate(
        [pairs.astype(jnp.float32), weights, rank.astype(jnp.float32)], axis=1
    )
    return table, slot, kept


def after(array, *others):
    return lax.optimization_barrier((array, *others))[0]


class Spread:
    def __init__(self, ring, parts):
        self.ring, self.parts = ring, parts
        self.now = {(i, step): part for i, part in enumerate(parts) for step in (1, -1)}
        self.came = {}

    def hop(self, h, orders=None, wait=()):
        ring = self.ring
        for (i, step), cur in self.now.items():
            if h == ring.packed:
                cur = product("pt,td->pd", orders[step], cur).astype(jnp.bfloat16)
            elif ring.rows(h) < cur.shape[0]:
                cur = cur[: ring.rows(h)]
            if wait:
                cur = after(cur, *wait)
            cur = ring.shift(cur, step)
            self.now[i, step] = cur
            self.came[i, step, h] = cur

    def at(self, h):
        return tuple(self.came[i, step, h] for (i, step) in self.now)

    def pick(self, choose):
        ring = self.ring
        halves = []
        for i, part in enumerate(self.parts):
            picked = []
            for back in range(ring.size):
                if back == 0:
                    block = part
                elif back == ring.half:
                    block = jnp.concatenate(
                        [self.came[i, 1, ring.half], self.came[i, -1, ring.half]], axis=0
                    )
                elif back < ring.half:
                    block = self.came[i, 1, back]
                else:
                    block = self.came[i, -1, ring.size - back]
                chosen = choose[back][:, : block.shape[0]]
                pace = min(back, ring.size - back) + 2
                if pace < ring.half:
                    chosen = after(chosen, self.came[i, 1, pace], self.came[i, -1, pace])
                picked.append(product("st,td->sd", chosen, block).astype(jnp.bfloat16))
            halves.append(jnp.stack(picked))
        return jnp.concatenate(halves, axis=-1)


class Collect:
    def __init__(self, ring, rows, choose, orders, batch):
        self.ring, self.choose, self.orders = ring, choose, orders
        self.parts = columns(rows)
        self.now = {(i, step): None for i in range(len(self.parts)) for step in (1, -1)}
        self.came = {}
        self.ready = None
        if batch:
            terms = product("bst,bsd->btd", choose, rows).astype(jnp.bfloat16)
            self.ready = [columns(terms[back]) for back in range(ring.size)]

    def term(self, i, back, first, count):
        if self.ready is not None:
            return self.ready[back][i][first : first + count].astype(jnp.float32)
        chosen = self.choose[back][:, first : first + count]
        return product("st,sd->td", chosen, self.parts[i][back])

    def hop(self, h, wait=()):
        ring = self.ring
        for (i, step), came in self.now.items():
            count = ring.rows(h)
            first = count if h == ring.half and step == -1 else 0
            total = self.term(i, (step * h) % ring.size, first, count)
            if came is not None:
                if h == ring.packed - 1:
                    total = total + product("pt,pd->td", self.orders[step], came)
                else:
                    wide = came.astype(jnp.float32)
                    total = total + jnp.pad(wide, ((0, count - wide.shape[0]), (0, 0)))
            total = total.astype(jnp.bfloat16)
            if wait:
                total = after(total, *wait)
            came = ring.shift(total, -step)
            self.now[i, step] = came
            self.came[i, step, h] = came

    def at(self, h):
        return tuple(self.came[i, step, h] for (i, step) in self.now)

    def result(self):
        done = []
        for i in range(len(self.parts)):
            local = self.term(i, 0, 0, self.ring.tok)
            both = self.now[i, 1].astype(jnp.float32) + self.now[i, -1].astype(jnp.float32)
            done.append((local + both).astype(jnp.bfloat16))
        return jnp.concatenate(done, axis=-1)


def exchange(array, mask):
    count = lax.axis_size("dp")
    return lax.ppermute(array, "dp", [(x, x ^ mask) for x in range(count)])


def columns(array):
    return jnp.split(array, PARTS, axis=-1)


def per_device(
    tokens,
    expert_ids,
    route_weights,
    cotangent,
    in_base,
    in_a,
    in_b,
    in_mag,
    out_base,
    out_a,
    out_b,
    out_mag,
):
    experts = lax.axis_size("expert")
    tok, top = expert_ids.shape
    width = tokens.shape[1]
    cap = tok * top // experts
    ring = Ring(experts, tok, cap)
    size = ring.size
    me = lax.axis_index("expert")
    z, core = me // CORES, me % CORES

    tok_ring = Spread(ring, columns(tokens))
    tok_ring.hop(1)
    table, slot, kept = route_tables(ring, expert_ids, route_weights, me)
    got = lax.all_to_all(
        table[:, None, :], "expert", split_axis=0, concat_axis=0, tiled=True
    )[:, 0]
    tok_ring.hop(2)
    tok_ring.hop(3)
    tok_ring.hop(4)
    got = after(got, *tok_ring.at(4))
    back = (z - jnp.arange(size, dtype=jnp.int32)) % size
    mine = got[back * CORES + core]
    other = got[back * CORES + 1 - core]
    places = mine[:, : CORES * cap].astype(jnp.int32)
    low, high = places[:, :cap], places[:, cap:]
    places = jnp.concatenate(
        [jnp.where(core == 0, low, high), jnp.where(core == 0, high, low)], axis=1
    )
    spots = jnp.arange(tok, dtype=jnp.int32)
    choose = (places[:, :, None] == spots[None, None, :]).astype(jnp.bfloat16)
    row_weights = jnp.concatenate(
        [
            mine[:, CORES * cap : (CORES + 1) * cap].reshape(-1),
            other[:, CORES * cap : (CORES + 1) * cap].reshape(-1),
        ]
    )
    ranks = mine[:, (CORES + 1) * cap :].astype(jnp.int32)
    span = jnp.arange(ring.rows(ring.packed), dtype=jnp.int32)
    orders = {
        step: (ranks[(step * (ring.packed - 1)) % size][None, :] == span[:, None]).astype(
            jnp.bfloat16
        )
        for step in (1, -1)
    }

    def swapped_in(picked):
        own = picked[:, :cap].reshape(size * cap, width)
        sent = ring.swap(picked[:, cap:].reshape(size * cap, width))
        return jnp.concatenate([own, sent], axis=0)

    def swapped_out(rows):
        own = rows[: size * cap].reshape(size, cap, width)
        swapped = ring.swap(rows[size * cap :]).reshape(size, cap, width)
        return jnp.concatenate([own, swapped], axis=1)

    for h in range(5, ring.packed + 1):
        tok_ring.hop(h, orders)
    weights_in = after(in_base[0], *tok_ring.at(ring.packed))
    weights_out = after(out_base[0], *tok_ring.at(ring.packed))
    norm_in = column_norms(weights_in, in_a[0], in_b[0])
    norm_out = column_norms(weights_out, out_a[0], out_b[0])
    params = (
        weights_in,
        in_a[0],
        in_b[0],
        in_mag[0] / norm_in,
        weights_out,
        out_a[0],
        out_b[0],
        out_mag[0] / norm_out,
    )
    cot_ring = Spread(ring, columns(after(cotangent, *tok_ring.at(ring.packed))))
    ahead = 0
    for h in range(ring.packed + 1, ring.half + 1):
        tok_ring.hop(h)
        ahead += 1
        cot_ring.hop(ahead)

    token_rows = swapped_in(tok_ring.pick(choose))
    result, saved = forward_rows(token_rows, params)
    hidden = saved[2]
    weighted = (row_weights[:, None] * result.astype(jnp.float32)).astype(jnp.bfloat16)
    mix_ring = Collect(ring, swapped_out(weighted), choose, orders, True)
    cot_ring.hop(3)
    cot_ring.hop(4)
    cot_ring.hop(5)
    cot_ring.hop(6, orders)
    cot_ring.hop(7, wait=(hidden,))
    cot_ring.hop(8, wait=(mix_ring.ready[size // 2][0],))
    mix_ring.hop(8)
    mix_ring.hop(7)
    mix_ring.hop(6)
    raw_cot = after(swapped_in(cot_ring.pick(choose)), *mix_ring.at(7)).astype(jnp.float32)
    cot_rows = (row_weights[:, None] * raw_cot).astype(jnp.bfloat16)
    input_grad, terms = backward_rows(saved, cot_rows, params, mix_ring)
    mix_ring.hop(3, wait=(input_grad,))
    mix_ring.hop(2)
    grad_rows = swapped_out(input_grad)
    grad_ring = Collect(ring, grad_rows, choose, orders, False)
    grad_ring.hop(8)
    mix_ring.hop(1, wait=(grad_rows,))

    for h in (7, 6, 5):
        grad_ring.hop(h)
    row_grad = jnp.sum(result.astype(jnp.float32) * raw_cot, axis=-1).reshape(CORES, size, cap)
    by_core = jnp.stack(
        [
            jnp.where(core == 0, row_grad[0], row_grad[1]),
            jnp.where(core == 0, row_grad[1], row_grad[0]),
        ],
        axis=1,
    )[back].reshape(experts, 1, cap)
    by_core = after(by_core, *grad_ring.at(6))
    returned = lax.all_to_all(by_core, "expert", split_axis=0, concat_axis=0, tiled=True)[:, 0]
    slots = jnp.arange(cap, dtype=jnp.int32)
    held = kept[:, :, None] & (slot[:, :, None] == slots[None, None, :])
    per_pair = jnp.sum(jnp.where(held, returned[:, None, :], 0.0), axis=2)
    every = jnp.arange(experts, dtype=jnp.int32)
    named = expert_ids[:, :, None] == every[None, None, :]
    route_grad = jnp.sum(jnp.where(named, per_pair.T[:, None, :], 0.0), axis=2)

    low_in, raw_in, hidden, low_out, raw_out = saved
    grad_out, back_out, grad_in, back_in, out_mag_rows, in_mag_rows = terms
    rank, inner = in_b.shape[2], in_b.shape[3]
    wide = jnp.concatenate(
        [
            product("nd,npr->prd", token_rows, back_in).reshape(-1, width),
            product("nr,nd->rd", low_out, grad_out),
            (jnp.sum(out_mag_rows, axis=0) / norm_out)[None],
        ],
        axis=0,
    ).astype(jnp.bfloat16)
    slim = jnp.concatenate(
        [
            product("npr,npf->prf", low_in, grad_in).reshape(-1, inner),
            product("nf,nr->rf", hidden, back_out),
            jnp.sum(in_mag_rows, axis=0) / norm_in,
        ],
        axis=0,
    ).astype(jnp.bfloat16)
    grad_ring.hop(4, wait=(wide, slim))
    order = [4, 3, 2, 1]
    mask = 1
    while mask < lax.axis_size("dp"):
        add_wide, add_slim = exchange(wide, mask), exchange(slim, mask)
        wide = wide.astype(jnp.float32) + add_wide.astype(jnp.float32)
        slim = slim.astype(jnp.float32) + add_slim.astype(jnp.float32)
        mask = 2 * mask + 1
        if mask < lax.axis_size("dp"):
            wide, slim = wide.astype(jnp.bfloat16), slim.astype(jnp.bfloat16)
            grad_ring.hop(3, wait=(add_wide, add_slim))
    grad_ring.hop(2)
    grad_ring.hop(1, wait=(add_wide, add_slim))
    pairs = CORES * rank
    summed = (
        wide[:pairs].reshape(2, rank, width).transpose(0, 2, 1),
        slim[:pairs].reshape(2, rank, inner),
        slim[-2:],
        slim[pairs : pairs + rank].T,
        wide[pairs : pairs + rank],
        wide[-1],
    )
    return (
        mix_ring.result(),
        grad_ring.result(),
        route_grad,
        *(array[None] for array in summed),
    )


def solution(mesh):
    in_specs = (
        P(("groups", "expert", "dp"), None),
        P(("groups", "expert", "dp"), None),
        P(("groups", "expert", "dp"), None),
        P(("groups", "expert", "dp"), None),
        P("expert", None, None, None),
        P(("groups", "expert"), None, None, None),
        P(("groups", "expert"), None, None, None),
        P(("groups", "expert"), None, None),
        P("expert", None, None),
        P(("groups", "expert"), None, None),
        P(("groups", "expert"), None, None),
        P(("groups", "expert"), None),
    )
    out_specs = (
        P(("groups", "expert", "dp"), None),
        P(("groups", "expert", "dp"), None),
        P(("groups", "expert", "dp"), None),
        P(("groups", "expert"), None, None, None),
        P(("groups", "expert"), None, None, None),
        P(("groups", "expert"), None, None),
        P(("groups", "expert"), None, None),
        P(("groups", "expert"), None, None),
        P(("groups", "expert"), None),
    )
    return jax.shard_map(
        per_device, mesh=mesh, in_specs=in_specs, out_specs=out_specs, check_vma=False
    )
```
